32 devices in a mesh: ctx: 4 (over y, x), tp: 8 (over z, core).
Axes of the slice: x: 2, y: 2, z: 4, core: 2. Of those that a mesh axis runs over, the one named last changes fastest.
Arguments:
- queries: bfloat16 [4096, 8192], P('ctx', 'tp'), may hold values from -64 to 64
- context_keys: bfloat16 [4096, 1024], P('ctx'), may hold values from -6 to 6
- context_values: bfloat16 [4096, 1024], P('ctx'), may hold values from -6 to 6
- positions: int32 [4096], P('ctx'), may hold values from 0 to 4095, as said below
- out_weight: bfloat16 [8192, 8192], P('tp'), may hold values from -0.5 to 0.5
- residual_in: bfloat16 [4096, 8192], P(('ctx', 'tp')), may hold values from -3 to 3
- norm_gain: float32 [8192], replicated, may hold values from 0.5 to 1.5
- static_scale: float32 [1], replicated, may hold values from 0.004 to 0.009
Outputs:
- hidden_out: bfloat16 [4096, 8192], P(('ctx', 'tp'))
- clipped: bfloat16 [4096, 8192], P(('ctx', 'tp'))
The draws below stay inside these ranges and needn't reach their ends.
Inputs may be any that keep to these rules, and one draw needn't show every extreme that they name: Rows fall into aligned runs of 512 rows that hold consecutive positions in increasing order; all positions together are a permutation of 0 to 4095.
All inputs are finite; a program needn't handle non-finite values.
Results may differ from the reference program's by a relative error of at most 0.017.
Values may be sent and summed in bfloat16 or wider, within the bound.
A program may use at most 128 MiB of HBM per device.

```python
import math
import jax
import jax.numpy as jnp
from jax import lax

D = 8192
HEADS = 64
KVH = 8
HD = 128
TOK_DEV = 1024
SPAN = 512
TOKENS = 4096
N_TP = 8


def span_order(key):
    return jax.random.permutation(jax.random.fold_in(key, 5), TOKENS // SPAN).astype(jnp.int32)


def row_positions(key):
    order = span_order(key)
    row_ids = jnp.arange(TOKENS, dtype=jnp.int32)
    return (order[row_ids // SPAN] * SPAN + row_ids % SPAN).astype(jnp.int32)


def shared_draw(key):
    base_key = jax.random.fold_in(key, 71)
    first_key, second_key = jax.random.split(base_key, 2)
    key_table = jnp.clip(jax.random.normal(first_key, (TOKENS, KVH * HD), jnp.float32), -6.0, 6.0)
    query_table = jnp.clip(1.5 * jax.random.normal(second_key, (TOKENS, HEADS * HD), jnp.float32), -9.0, 9.0)
    return (query_table, key_table)


def draw_queries(key, part):
    return shared_draw(key)[0].astype(jnp.bfloat16)


def draw_context_keys(key, part):
    return shared_draw(key)[1].astype(jnp.bfloat16)


def draw_positions(key, part):
    return row_positions(key)


def shard_levels(stream_key, dims, pieces, least, high):
    level = 1.0
    for dim, shards_of in pieces:
        steps = jax.random.uniform(jax.random.fold_in(jax.random.fold_in(stream_key, 6), dim), (shards_of,), jnp.float32, least / len(pieces), high / len(pieces))
        level = level * jnp.repeat(jnp.exp(steps), dims[dim] // shards_of).reshape((-1,) + (1,) * (len(dims) - 1 - dim))
    return level


def scatter_about(stream_key, shape, spread, most, pieces=(), kind=jnp.bfloat16):
    level = shard_levels(stream_key, shape, pieces, -0.22, 0.18) if pieces else 1.0
    entries = jax.random.normal(stream_key, shape, jnp.float32) * spread * level
    return jnp.minimum(jnp.maximum(entries, -most), most).astype(kind)


def setup_inputs(seed: int = 0) -> dict:
    key_of = jax.random.split(jax.random.key(seed), 9)
    queries = draw_queries(jax.random.fold_in(key_of[8], 71), 0)
    context_keys = draw_context_keys(jax.random.fold_in(key_of[8], 71), 0)
    context_values = scatter_about(key_of[2], (TOKENS, KVH * HD), 1.0, 6.0, ((0, 4),))
    positions = draw_positions(jax.random.fold_in(key_of[8], 71), 0)
    out_weight = scatter_about(key_of[4], (HEADS * HD, D), HD ** -0.5, 0.5, ((0, 8),))
    residual_in = scatter_about(key_of[5], (TOKENS, D), 0.5, 3.0, ((0, 32),))
    norm_gain = jnp.clip(1.0 + 0.1 * jax.random.normal(key_of[6], (D,), jnp.float32), 0.5, 1.5)
    static_scale = jnp.clip(jnp.exp(jax.random.uniform(key_of[7], (1,), jnp.float32, math.log(0.004), math.log(0.009))), 0.004, 0.009)
    return dict(queries=queries, context_keys=context_keys, context_values=context_values, positions=positions, out_weight=out_weight, residual_in=residual_in, norm_gain=norm_gain, static_scale=static_scale)


masked_fill = -1e+30

def attend_head(head, queries, context_keys, context_values, positions):
    kv_head = head // (HEADS // KVH)
    query_cols = lax.dynamic_slice_in_dim(queries, head * HD, HD, 1).astype(jnp.float32)
    key_cols = lax.dynamic_slice_in_dim(context_keys, kv_head * HD, HD, 1).astype(jnp.float32)
    value_cols = lax.dynamic_slice_in_dim(context_values, kv_head * HD, HD, 1).astype(jnp.float32)
    block_count = TOKENS // TOK_DEV

    def one_block(block_args):
        query_blk, query_pos = block_args
        scores = jnp.dot(query_blk, key_cols.T, preferred_element_type=jnp.float32, precision=lax.Precision.HIGHEST) * (1.0 / math.sqrt(HD))
        allowed = positions[None, :] <= query_pos[:, None]
        row_max = lax.optimization_barrier(jnp.max(jnp.where(allowed, scores, masked_fill), axis=1))
        expo = jnp.where(allowed, jnp.exp(scores - row_max[:, None]), 0.0)
        row_total = lax.optimization_barrier(jnp.sum(expo, axis=1))
        rounded = lax.optimization_barrier(expo.astype(jnp.bfloat16))
        output = jnp.dot(rounded.astype(jnp.float32), value_cols, preferred_element_type=jnp.float32, precision=lax.Precision.HIGHEST)
        return (output / row_total[:, None]).astype(jnp.bfloat16)
    finished = lax.map(one_block, (query_cols.reshape(block_count, TOK_DEV, HD), positions.reshape(block_count, TOK_DEV)))
    return finished.reshape(TOKENS, HD)

def reference(queries, context_keys, context_values, positions, out_weight, residual_in, norm_gain, static_scale):
    head_ids = jnp.arange(HEADS, dtype=jnp.int32)
    attended = lax.map(lambda head: attend_head(head, queries, context_keys, context_values, positions), head_ids)
    attended = jnp.transpose(attended, (1, 0, 2)).reshape(TOKENS, HEADS * HD)
    group_width = HEADS * HD // N_TP
    summed = residual_in.astype(jnp.float32)
    for group_index in range(N_TP):
        low_col = group_index * group_width
        group_term = jnp.dot(attended[:, low_col:low_col + group_width].astype(jnp.float32), out_weight[low_col:low_col + group_width].astype(jnp.float32), preferred_element_type=jnp.float32, precision=lax.Precision.HIGHEST)
        group_term = lax.optimization_barrier(group_term.astype(jnp.bfloat16))
        summed = summed + group_term.astype(jnp.float32)
    hidden_out = summed.astype(jnp.bfloat16)
    inv_rms = lax.rsqrt(lax.optimization_barrier(jnp.mean(summed * summed, axis=1, keepdims=True)) + 1e-05)
    limit = 448.0 * static_scale[0]
    clipped = jnp.clip(summed * inv_rms * norm_gain[None, :], -limit, limit).astype(jnp.bfloat16)
    return (hidden_out, clipped)
```

```python
import functools
import math

import jax
import jax.numpy as jnp
from jax import lax
from jax.experimental import pallas as pl
from jax.experimental.pallas import tpu as pltpu
from jax.sharding import PartitionSpec as P

KVH = 8
HD = 128
SPAN = 512
MESH_ID = pl.DeviceIdType.MESH


def gather_kernel(count, share_count, keys_ref, values_ref, pos_ref, kv_ref, pos_out, send_sem, recv_sem, own_sem):
    me = lax.axis_index("ctx")
    head = lax.axis_index("tp") // share_count
    cols = pl.ds(pl.multiple_of(head * HD, HD), HD)
    barrier = pltpu.get_barrier_semaphore()
    for step in range(1, count):
        pl.semaphore_signal(
            barrier, inc=1, device_id={"ctx": (me + step) % count}, device_id_type=MESH_ID
        )
    pl.semaphore_wait(barrier, count - 1)
    sources = (keys_ref.at[:, cols], values_ref.at[:, cols], pos_ref)
    rows = keys_ref.shape[0]
    here = pl.ds(pl.multiple_of(me * rows, rows), rows)
    targets = (kv_ref.at[0, here, :], kv_ref.at[1, here, :], pos_out.at[me])
    copies = []
    for step in range(1, count):
        for part in range(3):
            copy = pltpu.make_async_remote_copy(
                src_ref=sources[part],
                dst_ref=targets[part],
                send_sem=send_sem.at[step - 1, part],
                recv_sem=recv_sem.at[step - 1, part],
                device_id={"ctx": (me + step) % count},
                device_id_type=MESH_ID,
            )
            copy.start()
            copies.append(copy)
    own = []
    for part in range(3):
        copy = pltpu.make_async_copy(sources[part], targets[part], own_sem.at[part])
        copy.start()
        own.append(copy)
    for copy in own:
        copy.wait()
    for copy in copies:
        copy.wait()


def gather_context(keys, values, positions, count, share_count):
    rows = keys.shape[0]
    pos_tile = positions.reshape(rows // 128, 128)
    return pl.pallas_call(
        functools.partial(gather_kernel, count, share_count),
        out_shape=(
            jax.ShapeDtypeStruct((2, count * rows, HD), keys.dtype),
            jax.ShapeDtypeStruct((count,) + pos_tile.shape, jnp.int32),
        ),
        in_specs=[
            pl.BlockSpec(memory_space=pl.ANY),
            pl.BlockSpec(memory_space=pl.ANY),
            pl.BlockSpec(memory_space=pltpu.VMEM),
        ],
        out_specs=(pl.BlockSpec(memory_space=pltpu.VMEM), pl.BlockSpec(memory_space=pltpu.VMEM)),
        scratch_shapes=[
            pltpu.SemaphoreType.DMA((count - 1, 3)),
            pltpu.SemaphoreType.DMA((count - 1, 3)),
            pltpu.SemaphoreType.DMA((3,)),
        ],
        compiler_params=pltpu.CompilerParams(collective_id=0, has_side_effects=True),
    )(keys, values, pos_tile)


def attend_kernel(pair, order_ref, rank_ref, q_ref, kv_ref, o_ref, vext, acc):
    first = (pl.program_id(0) == 0) & (pl.program_id(1) == 0)

    @pl.when(first)
    def _():
        vext[:, :HD] = kv_ref[1]
        vext[:, HD:] = jnp.ones((vext.shape[0], HD), vext.dtype)

    rank = rank_ref[pl.program_id(0)]
    scale = math.log2(math.e) / math.sqrt(HD)

    def block(slot, maxes, masked):
        rows = pl.ds(pl.multiple_of(slot * SPAN, SPAN), SPAN)
        key_blk = kv_ref[0, rows, :]
        value_blk = vext[rows, :]
        if masked:
            query_id = lax.broadcasted_iota(jnp.int32, (SPAN, SPAN), 0)
            key_id = lax.broadcasted_iota(jnp.int32, (SPAN, SPAN), 1)
            allowed = key_id <= query_id
        out = []
        for h in range(pair):
            scores = lax.dot_general(
                q_ref[:, h * HD : (h + 1) * HD],
                key_blk,
                (((1,), (1,)), ((), ())),
                preferred_element_type=jnp.float32,
            )
            if masked:
                scores = jnp.where(allowed, scores, -1e30)
                new_max = jnp.max(scores, axis=1, keepdims=True)
            else:
                new_max = jnp.maximum(maxes[h], jnp.max(scores, axis=1, keepdims=True))
            weights = jnp.exp2((scores - new_max) * scale).astype(jnp.bfloat16)
            term = jnp.dot(weights, value_blk, preferred_element_type=jnp.float32)
            if masked:
                acc[h] = term
            else:
                acc[h] = acc[h] * jnp.exp2((maxes[h] - new_max) * scale) + term
            out.append(new_max)
        return tuple(out)

    maxes = block(order_ref[rank], None, True)
    lax.fori_loop(0, rank, lambda i, m: block(order_ref[i], m, False), maxes)
    for h in range(pair):
        o_ref[:, h * HD : (h + 1) * HD] = (acc[h, :, :HD] / acc[h, :, HD:]).astype(o_ref.dtype)


def attend(queries, kv, order, rank):
    rows, width = queries.shape
    pair = 2
    total = kv.shape[1]
    block = pl.BlockSpec((SPAN, pair * HD), lambda i, h, *_: (i, h))
    return pl.pallas_call(
        functools.partial(attend_kernel, pair),
        out_shape=jax.ShapeDtypeStruct((rows, width), queries.dtype),
        grid_spec=pltpu.PrefetchScalarGridSpec(
            num_scalar_prefetch=2,
            grid=(rows // SPAN, width // (pair * HD)),
            in_specs=[block, pl.BlockSpec((2, total, HD), lambda i, h, *_: (0, 0, 0))],
            out_specs=block,
            scratch_shapes=[
                pltpu.VMEM((total, 2 * HD), jnp.bfloat16),
                pltpu.VMEM((pair, SPAN, 2 * HD), jnp.float32),
            ],
        ),
        compiler_params=pltpu.CompilerParams(
            dimension_semantics=("arbitrary", "arbitrary"), vmem_limit_bytes=40 * 1024 * 1024
        ),
    )(order, rank, queries, kv)


def shards(
    queries,
    context_keys,
    context_values,
    positions,
    out_weight,
    residual_in,
    norm_gain,
    static_scale,
):
    ctx_count = lax.axis_size("ctx")
    tp_count = lax.axis_size("tp")
    share_count = tp_count // KVH
    kv, every_pos = gather_context(
        context_keys, context_values, positions, ctx_count, share_count
    )
    ranks = every_pos.reshape(-1, SPAN)[:, 0] // SPAN
    span_ids = jnp.arange(ranks.shape[0], dtype=jnp.int32)
    order = jnp.sum(jnp.where(ranks[None, :] == span_ids[:, None], span_ids[None, :], 0), axis=1)
    own_rank = positions.reshape(-1, SPAN)[:, 0] // SPAN
    attended = attend(queries, kv, order, own_rank)
    mine = lax.psum_scatter(
        jnp.dot(attended, out_weight, preferred_element_type=jnp.float32).astype(jnp.bfloat16),
        "tp",
        scatter_dimension=0,
        tiled=True,
    ).astype(jnp.float32)
    summed = residual_in.astype(jnp.float32) + mine
    hidden_out = summed.astype(jnp.bfloat16)
    inv_rms = lax.rsqrt(jnp.mean(summed * summed, axis=1, keepdims=True) + 1e-05)
    limit = 448.0 * static_scale[0]
    clipped = jnp.clip(summed * inv_rms * norm_gain[None, :], -limit, limit).astype(jnp.bfloat16)
    return (hidden_out, clipped)


def solution(mesh):
    return jax.shard_map(
        shards,
        mesh=mesh,
        in_specs=(
            P("ctx", "tp"),
            P("ctx", None),
            P("ctx", None),
            P("ctx"),
            P("tp", None),
            P(("ctx", "tp"), None),
            P(),
            P(),
        ),
        out_specs=(P(("ctx", "tp"), None), P(("ctx", "tp"), None)),
        check_vma=False,
    )
```
